32 devices in a mesh: dp: 16 (over z, y, core), space: 2 (over x).
Axes of the slice: x: 2, y: 2, z: 4, core: 2. Of those that a mesh axis runs over, the one named last changes fastest.
Arguments:
- feature_map: bfloat16 [16, 24, 84, 256], P('dp', 'space'), may hold values from -6 to 6
- proposals: int32 [16, 128, 4], P('dp'), may hold values from 0 to 84, as said below
- hidden_weight: bfloat16 [12544, 512], P(None, 'space'), may hold values from -0.0546875 to 0.0546875
- output_weight: bfloat16 [512, 512], P('space'), may hold values from -0.25 to 0.25
- upstream: bfloat16 [16, 128, 512], P('dp'), may hold values from -6 to 6
Outputs:
- hidden_weight_grad: float32 [12544, 512], P('dp', 'space')
- output_weight_grad: float32 [512, 512], P('space')
- feature_grad: float32 [16, 24, 84, 256], P('dp', 'space')
The draws below stay inside these ranges and needn't reach their ends.
Inputs may be any that keep to these rules, and one draw needn't show every extreme that they name: `proposals`: each row holds top, left, bottom, right with top < bottom <= 24 and left < right <= 84.
All inputs are finite; a program needn't handle non-finite values.
Results may differ from the reference program's by a relative error of at most 0.012.
Values may be sent and summed in bfloat16 or wider, within the bound.
No kernel may reach another device: no remote copies, remote signals or barrier semaphores. Data moves between devices by JAX's collectives and lax.ppermute only.
A program may use at most 128 MiB of HBM per device.

```python
import jax
import jax.numpy as jnp
from jax import lax

C = 256
POOL = 7
HID = 512
COLS = 84
HALF_ROWS = 12
ROIS = 128
CIN = 12544
IMAGES = 16


def draw_proposals(key, part):
    keys = jax.random.split(jax.random.fold_in(key, 11), 4)
    height_cells = 2 * HALF_ROWS
    top_edge = jax.random.randint(keys[0], (IMAGES, ROIS), 0, height_cells)
    tallness = jax.random.randint(keys[1], (IMAGES, ROIS), 1, height_cells + 1)
    left_edge = jax.random.randint(keys[2], (IMAGES, ROIS), 0, COLS)
    wideness = jax.random.randint(keys[3], (IMAGES, ROIS), 1, COLS + 1)
    bottom_edge = jnp.minimum(top_edge + tallness, height_cells)
    right_edge = jnp.minimum(left_edge + wideness, COLS)
    return jnp.stack([top_edge, left_edge, bottom_edge, right_edge], axis=-1).astype(jnp.int32)


def block_scale(stream_key, dims, pieces, low, largest):
    level, own = 1.0, jax.random.fold_in(stream_key, 6)
    for axis_at, shards_of in pieces:
        draws = jnp.exp(jax.random.uniform(jax.random.fold_in(own, axis_at), (shards_of,), jnp.float32, low / len(pieces), largest / len(pieces)))
        level = level * jnp.repeat(draws, dims[axis_at] // shards_of).reshape([-1 if axis == axis_at else 1 for axis in range(len(dims))])
    return level


def normal_values(rng, extent, scale, bound, cuts=(), dtype=jnp.bfloat16):
    factor_of = block_scale(rng, extent, cuts, -0.22, 0.18) if cuts else 1.0
    values = jax.random.normal(rng, extent, jnp.float32) * scale * factor_of
    return jnp.minimum(jnp.maximum(values, -bound), bound).astype(dtype)


def setup_inputs(seed: int = 0) -> dict:
    streams_of = jax.random.split(jax.random.key(seed), 6)
    return {
        "feature_map": normal_values(streams_of[0], (IMAGES, 2 * HALF_ROWS, COLS, C), 1.0, 6.0, ((0, 16), (1, 2))),
        "proposals": draw_proposals(jax.random.fold_in(streams_of[5], 71), 0),
        "hidden_weight": normal_values(streams_of[2], (CIN, HID), CIN ** -0.5, 0.0546875, ((1, 2),)),
        "output_weight": normal_values(streams_of[3], (HID, HID), HID ** -0.5, 0.25, ((0, 2),)),
        "upstream": normal_values(streams_of[4], (IMAGES, ROIS, HID), 1.0, 6.0, ((0, 16),)),
    }


def axis_weights(low_edge, high_edge, grid_points):
    edge_start = low_edge.astype(jnp.float32)
    bin_size = (high_edge - low_edge).astype(jnp.float32) / POOL
    bin_index = jnp.arange(POOL).astype(jnp.float32)
    offsets = jnp.array([0.25, 0.75], jnp.float32)
    sample_points = edge_start[:, None, None] + (bin_index[None, :, None] + offsets[None, None, :]) * bin_size[:, None, None] - 0.5
    weights = jnp.maximum(0.0, 1.0 - jnp.abs(sample_points[..., None] - grid_points[None, None, None, :]))
    return lax.optimization_barrier(jnp.mean(weights, axis=2))

def activate(values):
    return jax.nn.gelu(values, approximate=True)

def gelu_grad(values, incoming):
    return jax.vjp(activate, values)[1](incoming)[0]

def crop_rows(own_map, row_weight, col_weight):
    height_cells, width_cells, channels = own_map.shape
    proposal_count = row_weight.shape[0]
    flattened = jnp.transpose(own_map, (1, 0, 2)).reshape(width_cells, height_cells * channels)
    across = jnp.dot(col_weight.reshape(proposal_count * POOL, width_cells), flattened, preferred_element_type=jnp.float32)
    across = across.reshape(proposal_count, POOL, height_cells, channels)
    pooled = jnp.einsum('riy,rjyc->rijc', row_weight.astype(jnp.float32), across, precision=lax.Precision.HIGHEST)
    return pooled.reshape(proposal_count, POOL * POOL * channels)

def crop_back(grad_pooled, row_weight, col_weight, channels):
    proposal_count, _, height_cells = row_weight.shape
    width_cells = col_weight.shape[2]
    grad_block = grad_pooled.astype(jnp.float32).reshape(proposal_count, POOL, POOL, channels)
    spread = jnp.einsum('riy,rijc->rjyc', row_weight.astype(jnp.float32), grad_block, precision=lax.Precision.HIGHEST)
    total = lax.dot_general(col_weight.astype(jnp.float32).reshape(proposal_count * POOL, width_cells), spread.reshape(proposal_count * POOL, height_cells * channels), (((0,), (0,)), ((), ())), precision=lax.Precision.HIGHEST, preferred_element_type=jnp.float32)
    return jnp.transpose(total.reshape(width_cells, height_cells, channels), (1, 0, 2))

def reference(feature_map, proposals, hidden_weight, output_weight, upstream):

    def per_image(running, sample):
        own_map, corners, incoming = sample
        height_cells = own_map.shape[0]
        row_weight = axis_weights(corners[:, 0], corners[:, 2], jnp.arange(height_cells).astype(jnp.float32))
        col_weight = axis_weights(corners[:, 1], corners[:, 3], jnp.arange(COLS).astype(jnp.float32)).astype(jnp.bfloat16)
        pooled = crop_rows(own_map, row_weight, col_weight).astype(jnp.bfloat16)
        pre_hidden = jnp.dot(pooled, hidden_weight, preferred_element_type=jnp.float32)
        hidden = activate(pre_hidden).astype(jnp.bfloat16)
        pre_output = jnp.dot(hidden, output_weight, preferred_element_type=jnp.float32)
        output_delta = gelu_grad(pre_output, incoming.astype(jnp.float32)).astype(jnp.bfloat16)
        step_second = lax.dot_general(hidden, output_delta, (((0,), (0,)), ((), ())), preferred_element_type=jnp.float32)
        hidden_back = lax.dot_general(output_delta, output_weight, (((1,), (1,)), ((), ())), preferred_element_type=jnp.float32)
        hidden_delta = gelu_grad(pre_hidden, hidden_back).astype(jnp.bfloat16)
        step_first = lax.dot_general(pooled, hidden_delta, (((0,), (0,)), ((), ())), preferred_element_type=jnp.float32)
        pooled_grad = lax.dot_general(hidden_delta, hidden_weight, (((1,), (1,)), ((), ())), preferred_element_type=jnp.float32)
        map_grad = crop_back(pooled_grad, row_weight, col_weight, own_map.shape[2])
        return ((running[0] + step_first, running[1] + step_second), map_grad)
    start = (jnp.zeros((CIN, HID), jnp.float32), jnp.zeros((HID, HID), jnp.float32))
    totals, feature_grad = lax.scan(per_image, start, (feature_map, proposals, upstream))
    return (totals[0], totals[1], feature_grad)
```

```python
import jax
import jax.numpy as jnp
from jax import lax
from jax.experimental import pallas as pl
from jax.experimental.pallas import tpu as pltpu
from jax.sharding import PartitionSpec as P

POOL = 7
BINS = POOL * POOL
F32 = jnp.float32
BF16 = jnp.bfloat16


def activate(values):
    return jax.nn.gelu(values, approximate=True)


def gelu_grad(values, incoming):
    return jax.vjp(activate, values)[1](incoming)[0]


def sample_points(low_edge, high_edge):
    edge_start = low_edge.astype(F32)
    bin_size = (high_edge - low_edge).astype(F32) / POOL
    bin_index = jnp.arange(POOL).astype(F32)
    return [
        edge_start[None, :] + (bin_index[:, None] + offset) * bin_size[None, :] - 0.5
        for offset in (0.25, 0.75)
    ]


def tent(points, grid):
    return 0.5 * (
        jnp.maximum(0.0, 1.0 - jnp.abs(points[0] - grid))
        + jnp.maximum(0.0, 1.0 - jnp.abs(points[1] - grid))
    )


def dot(a, b, dims=((1,), (0,))):
    return lax.dot_general(a, b, (dims, ((), ())), preferred_element_type=F32)


def params(grid_rank, **more):
    return pltpu.CompilerParams(
        dimension_semantics=("arbitrary",) * grid_rank, vmem_limit_bytes=60 * 2**20, **more
    )


def crop_forward(row_tab, col_tab, map_own, map_other, weight, owners):
    _, rois, cells = row_tab.shape
    half_cells, channels = map_own.shape
    hidden = weight.shape[1]
    half = rois // 2
    owned = BINS * channels // owners
    part = owned // 2
    aligned = owned % 16 == 0

    def body(row_ref, col_ref, own_ref, other_ref, weight_ref, eye_ref, pre_ref, pack_ref, w2, crops_t):
        i = pl.program_id(0)
        row = row_ref[0]
        for j in range(POOL):
            w2[j * rois : (j + 1) * rois, :] = row * col_ref[j]
        pooled = (
            dot(w2[:, :half_cells], own_ref[...]) + dot(w2[:, half_cells:], other_ref[...])
        ).astype(BF16)
        acc = jnp.zeros((rois, hidden), F32)
        for j in range(POOL):
            crop = pooled[j * rois : (j + 1) * rois]
            acc += dot(crop, weight_ref[j * channels : (j + 1) * channels, :])
            twice = jnp.concatenate([crop[:half], crop[:half]], axis=0)
            start = pl.multiple_of((i * POOL + j) * channels, channels)
            crops_t[pl.ds(start, channels), :] = dot(eye_ref[...], twice, ((1,), (1,)))

        @pl.when(i == 0)
        def _():
            pre_ref[...] = acc

        @pl.when(i > 0)
        def _():
            pre_ref[...] += acc

        if not aligned:
            start = pl.multiple_of(i * (POOL * channels), channels)
            pack_ref[...] = crops_t[pl.ds(start, POOL * channels), :].astype(BF16)
            return

        @pl.when(i == POOL - 1)
        def _():
            left = lax.broadcasted_iota(jnp.int32, (part, 2 * half), 1) < half

            def pack(e, carry):
                start = pl.multiple_of(e * owned, 8)
                first = crops_t[pl.ds(start, part), :]
                second = crops_t[pl.ds(start + part, part), :]
                pack_ref[e] = jnp.where(left, first, second).astype(BF16)
                return carry

            lax.fori_loop(0, owners, pack, 0)

    whole = lambda *shape: pl.BlockSpec(shape, lambda i: (0,) * len(shape))
    if aligned:
        pack_spec, pack_shape = whole(owners, part, 2 * half), (owners, part, 2 * half)
    else:
        pack_spec = pl.BlockSpec((POOL * channels, 2 * half), lambda i: (i, 0))
        pack_shape = (BINS * channels, 2 * half)
    pre_hidden, packed = pl.pallas_call(
        body,
        grid=(POOL,),
        in_specs=[
            pl.BlockSpec((1, rois, cells), lambda i: (i, 0, 0)),
            whole(POOL, rois, cells),
            whole(half_cells, channels),
            whole(half_cells, channels),
            pl.BlockSpec((POOL * channels, hidden), lambda i: (i, 0)),
            whole(channels, channels),
        ],
        out_specs=[whole(rois, hidden), pack_spec],
        out_shape=[
            jax.ShapeDtypeStruct((rois, hidden), F32),
            jax.ShapeDtypeStruct(pack_shape, BF16),
        ],
        scratch_shapes=[
            pltpu.VMEM((POOL * rois, cells), BF16),
            pltpu.VMEM((BINS * channels, 2 * half), F32),
        ],
        compiler_params=params(1),
        cost_estimate=pl.CostEstimate(
            flops=2 * BINS * rois * cells * channels, transcendentals=0, bytes_accessed=20 * 2**20
        ),
        name="crop_forward",
    )(row_tab, col_tab, map_own, map_other, weight, jnp.eye(channels, dtype=BF16))
    if not aligned:
        packed = packed[:, :half].reshape(owners, owned, half)
    return pre_hidden, packed


def head(pre_own, pre_received, out_own, out_other, upstream):
    rois, hidden = pre_own.shape
    outputs = out_own.shape[1]
    half = rois // 2

    def body(own_ref, recv_ref, wown_ref, wother_ref, up_ref, hd_ref, mine_ref, grad_ref):
        pre_a = own_ref[...]
        pre_b = jnp.concatenate([recv_ref[half:], recv_ref[:half]], axis=0).astype(F32)
        hid_a = activate(pre_a).astype(BF16)
        hid_b = activate(pre_b).astype(BF16)
        pre_output = dot(hid_a, wown_ref[...]) + dot(hid_b, wother_ref[...])
        delta = gelu_grad(pre_output, up_ref[...].astype(F32)).astype(BF16)
        grad_ref[...] = dot(hid_a, delta, ((0,), (0,)))
        hd_a = gelu_grad(pre_a, dot(delta, wown_ref[...], ((1,), (1,)))).astype(BF16)
        hd_b = gelu_grad(
            pre_b[:half], dot(delta[:half], wother_ref[...], ((1,), (1,)))
        ).astype(BF16)
        hd_ref[...] = hd_a
        mine_ref[:, :hidden] = hd_a[:half]
        mine_ref[:, hidden:] = hd_b

    return pl.pallas_call(
        body,
        out_shape=[
            jax.ShapeDtypeStruct((rois, hidden), BF16),
            jax.ShapeDtypeStruct((half, 2 * hidden), BF16),
            jax.ShapeDtypeStruct((hidden, outputs), F32),
        ],
        compiler_params=pltpu.CompilerParams(vmem_limit_bytes=32 * 2**20),
        cost_estimate=pl.CostEstimate(flops=2 * 10**9, transcendentals=0, bytes_accessed=2**21),
        name="head",
    )(pre_own, pre_received, out_own, out_other, upstream)


def crop_backward_other(row_tab, col_tab, delta, weight):
    _, cells, rois = row_tab.shape
    hidden = weight.shape[1]
    channels = weight.shape[0] // BINS
    half_cells = cells // 2

    def body(row_ref, col_ref, delta_ref, weight_ref, crop_ref, out_ref, w2, acc):
        i = pl.program_id(0)
        row = row_ref[0]
        for j in range(POOL):
            w2[:, j * rois : (j + 1) * rois] = row * col_ref[j]
            crop_ref[j * rois : (j + 1) * rois, :] = dot(
                delta_ref[...], weight_ref[j * channels : (j + 1) * channels, :], ((1,), (1,))
            ).astype(BF16)
        part = dot(w2[...], crop_ref[...])

        @pl.when(i == 0)
        def _():
            acc[...] = part

        @pl.when(i > 0)
        def _():
            acc[...] += part

        @pl.when(i == POOL - 1)
        def _():
            out_ref[...] = acc[...].astype(BF16)

    return pl.pallas_call(
        body,
        grid=(POOL,),
        in_specs=[
            pl.BlockSpec((1, half_cells, rois), lambda i: (i, 1, 0)),
            pl.BlockSpec((POOL, half_cells, rois), lambda i: (0, 1, 0)),
            pl.BlockSpec((rois, hidden), lambda i: (0, 0)),
            pl.BlockSpec((POOL * channels, hidden), lambda i: (i, 0)),
        ],
        out_specs=[
            pl.BlockSpec((POOL * rois, channels), lambda i: (i, 0)),
            pl.BlockSpec((half_cells, channels), lambda i: (0, 0)),
        ],
        out_shape=[
            jax.ShapeDtypeStruct((BINS * rois, channels), BF16),
            jax.ShapeDtypeStruct((half_cells, channels), BF16),
        ],
        scratch_shapes=[
            pltpu.VMEM((half_cells, POOL * rois), BF16),
            pltpu.VMEM((half_cells, channels), F32),
        ],
        compiler_params=params(1),
        cost_estimate=pl.CostEstimate(
            flops=BINS * rois * cells * channels, transcendentals=0, bytes_accessed=14 * 2**20
        ),
        name="crop_backward_other",
    )(row_tab, col_tab, delta, weight)


def crop_backward_own(row_tab, col_tab, crops):
    _, cells, rois = row_tab.shape
    channels = crops.shape[1]
    half_cells = cells // 2

    def body(row_ref, col_ref, crop_ref, out_ref, w2):
        i = pl.program_id(0)
        row = row_ref[0]
        for j in range(POOL):
            w2[:, j * rois : (j + 1) * rois] = row * col_ref[j]
        part = dot(w2[...], crop_ref[...])

        @pl.when(i == 0)
        def _():
            out_ref[...] = part

        @pl.when(i > 0)
        def _():
            out_ref[...] += part

    return pl.pallas_call(
        body,
        grid=(POOL,),
        in_specs=[
            pl.BlockSpec((1, half_cells, rois), lambda i: (i, 0, 0)),
            pl.BlockSpec((POOL, half_cells, rois), lambda i: (0, 0, 0)),
            pl.BlockSpec((POOL * rois, channels), lambda i: (i, 0)),
        ],
        out_specs=pl.BlockSpec((half_cells, channels), lambda i: (0, 0)),
        out_shape=jax.ShapeDtypeStruct((half_cells, channels), F32),
        scratch_shapes=[pltpu.VMEM((half_cells, POOL * rois), BF16)],
        compiler_params=params(1),
        cost_estimate=pl.CostEstimate(
            flops=BINS * rois * cells * channels, transcendentals=0, bytes_accessed=9 * 2**20
        ),
        name="crop_backward_own",
    )(row_tab, col_tab, crops)


def weight_grad(packed, deltas, order, me):
    images, part, lanes = packed.shape
    half, width = deltas.shape[1:]
    hidden = width // 2
    if lanes == half:
        place = jnp.array([order[m] for m in range(images)])
        in_order = deltas[place[jnp.arange(images) ^ me]]
        total = jnp.einsum("mpr,mrh->ph", packed, in_order, preferred_element_type=F32)
        return total[:, :hidden], total[:, hidden:].astype(BF16)

    def body(me_ref, packed_ref, delta_ref, own_ref, other_ref):
        left = lax.broadcasted_iota(jnp.int32, (part, lanes), 1) < half
        tops = jnp.zeros((part, width), F32)
        bottoms = jnp.zeros((part, width), F32)
        for m in range(0, images, 2):
            a = packed_ref[me_ref[0] ^ m]
            b = packed_ref[me_ref[0] ^ (m + 1)]
            pair = jnp.concatenate([delta_ref[order[m]], delta_ref[order[m + 1]]], axis=0)
            a, b = a.astype(F32), b.astype(F32)
            top = jnp.where(left, a, pltpu.roll(b, half, 1)).astype(BF16)
            bottom = jnp.where(left, pltpu.roll(a, half, 1), b).astype(BF16)
            tops += dot(top, pair)
            bottoms += dot(bottom, pair)
        own_ref[:part] = tops[:, :hidden]
        own_ref[part:] = bottoms[:, :hidden]
        other_ref[:part] = tops[:, hidden:].astype(BF16)
        other_ref[part:] = bottoms[:, hidden:].astype(BF16)

    return pl.pallas_call(
        body,
        in_specs=[
            pl.BlockSpec(memory_space=pltpu.SMEM),
            pl.BlockSpec(memory_space=pltpu.VMEM),
            pl.BlockSpec(memory_space=pltpu.VMEM),
        ],
        out_shape=[
            jax.ShapeDtypeStruct((2 * part, hidden), F32),
            jax.ShapeDtypeStruct((2 * part, hidden), BF16),
        ],
        compiler_params=pltpu.CompilerParams(vmem_limit_bytes=48 * 2**20),
        cost_estimate=pl.CostEstimate(
            flops=4 * part * images * half * width, transcendentals=0, bytes_accessed=5 * 2**20
        ),
        name="weight_grad",
    )(me.reshape(1), packed, deltas)


def swap_space(values):
    size = lax.axis_size("space")
    return lax.ppermute(values, "space", [(k, size - 1 - k) for k in range(size)])


def swap_images(values, distance):
    return lax.ppermute(values, "dp", [(k, k ^ distance) for k in range(lax.axis_size("dp"))])


def on_device(feature_map, proposals, hidden_weight, output_weight, upstream):
    images = lax.axis_size("dp")
    assert lax.axis_size("space") == 2 and images & (images - 1) == 0
    own_map = feature_map[0]
    own_height, map_width, channels = own_map.shape
    rois = proposals.shape[1]
    side = lax.axis_index("space")
    me = lax.axis_index("dp").astype(jnp.int32)
    map_own = own_map.reshape(own_height * map_width, channels)
    map_other = swap_space(map_own)
    out_other = swap_space(output_weight)

    corners = jnp.roll(proposals[0], side * (rois // 2), axis=0)
    incoming = jnp.roll(upstream[0], side * (rois // 2), axis=0)

    cell = jnp.arange(2 * own_height * map_width, dtype=jnp.int32)
    row_in_order = cell // map_width
    grid_y = ((row_in_order + side * own_height) % (2 * own_height)).astype(F32)
    grid_x = (cell % map_width).astype(F32)
    ys = sample_points(corners[:, 0], corners[:, 2])
    xs = sample_points(corners[:, 1], corners[:, 3])
    lanes = lambda pts: [p[:, :, None] for p in pts]
    rows = lambda pts: [p[:, None, :] for p in pts]
    row_tab = tent(lanes(ys), grid_y[None, None, :]).astype(BF16)
    col_tab = tent(lanes(xs), grid_x[None, None, :]).astype(BF16)
    row_tab_t = tent(rows(ys), grid_y[None, :, None]).astype(BF16)
    col_tab_t = tent(rows(xs), grid_x[None, :, None]).astype(BF16)

    pre_hidden, packed = crop_forward(row_tab, col_tab, map_own, map_other, hidden_weight, images)
    pre_other = swap_space(pre_hidden.astype(BF16))
    received = lax.all_to_all(packed, "dp", 0, 0, tiled=True)
    delta, mine, second = head(pre_hidden, pre_other, output_weight, out_other, incoming)

    bits = images.bit_length() - 1
    gathered = mine[None]
    place = [0]
    for distance in [1 << b for b in range(bits - 1, -1, -1)]:
        gathered = jnp.concatenate([gathered, swap_images(gathered, distance)], axis=0)
        place = place + [p ^ distance for p in place]
    order = {m: k for k, m in enumerate(place)}

    crops, grad_other = crop_backward_other(row_tab_t, col_tab_t, delta, hidden_weight)
    grad_received = swap_space(grad_other)
    grad_own = crop_backward_own(row_tab_t, col_tab_t, crops)
    map_grad = (grad_own + grad_received.astype(F32)).reshape(own_height, map_width, channels)

    for distance in [1 << b for b in range(bits)]:
        rounded = second.astype(BF16)
        second = rounded.astype(F32) + swap_images(rounded, distance).astype(F32)

    first_own, first_other = weight_grad(received, gathered, order, me)
    first_total = first_own + swap_space(first_other).astype(F32)
    return (first_total, second, map_grad[None])


def solution(mesh):
    placed = (
        P("dp", "space", None, None),
        P("dp", None, None),
        P(None, "space"),
        P("space", None),
        P("dp", None, None),
    )
    return jax.shard_map(
        on_device,
        mesh=mesh,
        in_specs=placed,
        out_specs=(P("dp", "space"), P("space", None), P("dp", "space", None, None)),
        check_vma=False,
    )
```

```python
import jax
import jax.numpy as jnp
from jax import lax
from jax.experimental import pallas as pl
from jax.experimental.pallas import tpu as pltpu
from jax.sharding import PartitionSpec as P


POOL = 7
BINS = POOL * POOL
F32 = jnp.float32
BF16 = jnp.bfloat16


def activate(values):
    return jax.nn.gelu(values, approximate=True)


def gelu_grad(values, incoming):
    return jax.vjp(activate, values)[1](incoming)[0]


def sample_points(low_edge, high_edge):
    edge_start = low_edge.astype(F32)
    bin_size = (high_edge - low_edge).astype(F32) / POOL
    bin_index = jnp.arange(POOL).astype(F32)
    return [
        edge_start[None, :] + (bin_index[:, None] + offset) * bin_size[None, :] - 0.5
        for offset in (0.25, 0.75)
    ]


def tent(first, second, grid):
    return 0.5 * (
        jnp.maximum(0.0, 1.0 - jnp.abs(first - grid))
        + jnp.maximum(0.0, 1.0 - jnp.abs(second - grid))
    )


def dot(a, b, dims=((1,), (0,))):
    return lax.dot_general(a, b, (dims, ((), ())), preferred_element_type=F32)


LIMIT = 13
TAPS = 128


def kernel(body, out_shape, scratch=(), flops=10**9, limit=LIMIT, smem_first=False, anywhere=(), hbm_out=False):
    def call(*args):
        specs = [pl.BlockSpec(memory_space=pltpu.VMEM) for _ in args]
        if smem_first:
            specs[0] = pl.BlockSpec(memory_space=pltpu.SMEM)
        args = list(args)
        for k in anywhere:
            args[k] = pltpu.with_memory_space_constraint(args[k], pltpu.HBM)
            specs[k] = pl.BlockSpec(memory_space=pltpu.HBM)
        out_space = pltpu.HBM if hbm_out else pltpu.VMEM
        return pl.pallas_call(
            body,
            in_specs=specs,
            out_specs=jax.tree.map(lambda _: pl.BlockSpec(memory_space=out_space), out_shape),
            out_shape=out_shape,
            scratch_shapes=scratch,
            compiler_params=pltpu.CompilerParams(vmem_limit_bytes=limit * 2**20),
            cost_estimate=pl.CostEstimate(
                flops=int(flops), transcendentals=0, bytes_accessed=2**20
            ),
        )(*args)

    return call


def fetch(source, target, sems):
    rows = target.shape[0] // POOL
    copies = []
    for k in range(POOL):
        at = pl.ds(k * rows, rows)
        copies.append(pltpu.make_async_copy(source.at[at], target.at[at], sems.at[k]))
        copies[-1].start()
    return copies


def shaped(dtype, *shape):
    return jax.ShapeDtypeStruct(shape, dtype)


def spread(taps, cells, width, real, transposed=False):
    shape = (cells, 1) if transposed else (1, cells)
    cell = lax.broadcasted_iota(jnp.int32, shape, 0 if transposed else 1).astype(F32)
    row = jnp.floor((cell + 0.5) * (1.0 / width))
    column = jnp.where(cell < real, cell - row * width, -1.0)
    row = jnp.where(cell < real, row, -1.0)
    full = (cells, taps) if transposed else (taps, cells)
    tap = lax.broadcasted_iota(jnp.int32, full, 1 if transposed else 0).astype(F32)
    one = lambda where: jnp.where(tap == where, 1.0, 0.0).astype(BF16)
    return one(column), one(row)


def crop_own(points, map_own, width, real):
    count = points.shape[0]
    rois = count // POOL
    cells, channels = map_own.shape

    def body(pts, map_ref, col_ref, other_ref, part_ref, own_ref, w_a, w_b):
        sx, sy = spread(TAPS, cells, width, real)
        grid = lax.broadcasted_iota(jnp.int32, (count, TAPS), 1).astype(F32)
        weights = [tent(pts[:, k : k + 1], pts[:, k + 1 : k + 2], grid).astype(BF16) for k in (0, 2, 4)]
        col_ref[...] = dot(weights[0], sx).astype(BF16)
        own_ref[...] = dot(weights[1], sy).astype(BF16)
        other_ref[...] = dot(weights[2], sy).astype(BF16)
        for i in range(POOL):
            w2 = (w_a, w_b)[i % 2]
            for j in range(POOL):
                at = slice(j * rois, (j + 1) * rois)
                w2[at, :] = own_ref[i * rois : (i + 1) * rois, :] * col_ref[at, :]
            part_ref[i * count : (i + 1) * count, :] = dot(w2[...], map_ref[...])

    table = shaped(BF16, count, cells)
    return kernel(
        body,
        [table, table, shaped(F32, POOL * count, channels)],
        [pltpu.VMEM((count, cells), BF16)] * 3,
        2 * BINS * rois * cells * channels,
        limit=20,
    )(points, map_own)


def crop_all(col, row, map_other, partial, weight, owners):
    count, cells = col.shape
    rois = count // POOL
    half = rois // 2
    channels = map_other.shape[1]
    hidden = weight.shape[1]
    owned = BINS * channels // owners
    part = owned // 2
    aligned = owned % 16 == 0

    def body(col_ref, row_ref, map_ref, partial_ref, weight_ref, pre_ref, send_ref, pack_ref, w_a, w_b, crops_t):
        ahead = lax.broadcasted_iota(jnp.int32, (channels, channels), 0)
        eye = (ahead == lax.broadcasted_iota(jnp.int32, (channels, channels), 1)).astype(BF16)
        acc = jnp.zeros((rois, hidden), F32)
        for i in range(POOL):
            w2 = (w_a, w_b)[i % 2]
            for j in range(POOL):
                at = slice(j * rois, (j + 1) * rois)
                w2[at, :] = row_ref[i * rois : (i + 1) * rois, :] * col_ref[at, :]
            block = slice(i * count, (i + 1) * count)
            pooled = (partial_ref[block, :] + dot(w2[...], map_ref[...])).astype(BF16)
            for j in range(POOL):
                crop = pooled[j * rois : (j + 1) * rois]
                rows = slice((i * POOL + j) * channels, (i * POOL + j + 1) * channels)
                acc += dot(crop, weight_ref[rows, :])
                twice = jnp.concatenate([crop[:half], crop[:half]], axis=0)
                crops_t[rows, :] = dot(eye, twice, ((1,), (1,)))
        pre_ref[...] = acc
        send_ref[...] = acc.astype(BF16)
        if aligned:
            left = lax.broadcasted_iota(jnp.int32, (part, 2 * half), 1) < half
            for e in range(owners):
                first = crops_t[e * owned : e * owned + part, :]
                second = crops_t[e * owned + part : (e + 1) * owned, :]
                pack_ref[e] = jnp.where(left, first, second).astype(BF16)
        else:
            pack_ref[...] = crops_t[...].astype(BF16)

    pack = (owners, part, 2 * half) if aligned else (BINS * channels, 2 * half)
    pre_hidden, sent, packed = kernel(
        body,
        [shaped(F32, rois, hidden), shaped(BF16, rois, hidden), shaped(BF16, *pack)],
        [pltpu.VMEM((count, cells), BF16)] * 2
        + [pltpu.VMEM((BINS * channels, 2 * half), F32)],
        2 * BINS * rois * cells * channels,
        limit=32,
    )(col, row, map_other, partial, weight)
    if not aligned:
        packed = packed[:, :half].reshape(owners, owned, half)
    return pre_hidden, sent, packed


def head(pre_own, pre_received, out_own, out_other, upstream):
    rois, hidden = pre_own.shape
    outputs = out_own.shape[1]
    half = rois // 2

    def body(own_ref, recv_ref, wown_ref, wother_ref, up_ref, hd_ref, mine_ref, grad_ref):
        pre_a = own_ref[...]
        pre_b = jnp.concatenate([recv_ref[half:], recv_ref[:half]], axis=0).astype(F32)
        hid_a = activate(pre_a).astype(BF16)
        hid_b = activate(pre_b).astype(BF16)
        pre_output = dot(hid_a, wown_ref[...]) + dot(hid_b, wother_ref[...])
        delta = gelu_grad(pre_output, up_ref[...].astype(F32)).astype(BF16)
        grad_ref[...] = dot(hid_a, delta, ((0,), (0,)))
        hd_a = gelu_grad(pre_a, dot(delta, wown_ref[...], ((1,), (1,)))).astype(BF16)
        hd_b = gelu_grad(
            pre_b[:half], dot(delta[:half], wother_ref[...], ((1,), (1,)))
        ).astype(BF16)
        hd_ref[...] = hd_a
        mine_ref[:, :hidden] = hd_a[:half]
        mine_ref[:, hidden:] = hd_b

    return pl.pallas_call(
        body,
        out_shape=[
            jax.ShapeDtypeStruct((rois, hidden), BF16),
            jax.ShapeDtypeStruct((half, 2 * hidden), BF16),
            jax.ShapeDtypeStruct((hidden, outputs), F32),
        ],
        compiler_params=pltpu.CompilerParams(vmem_limit_bytes=8 * 2**20),
        cost_estimate=pl.CostEstimate(flops=2 * 10**9, transcendentals=0, bytes_accessed=2**21),
        name="head",
    )(pre_own, pre_received, out_own, out_other, upstream)


def tables_t(pts, which, cells, width, rows_ref, cols_ref):
    pts = pts[...]
    sx, sy = spread(TAPS, cells, width, cells, transposed=True)
    grid = lax.broadcasted_iota(jnp.int32, (TAPS, pts.shape[1]), 0).astype(F32)
    cols_ref[...] = dot(sx, tent(pts[0:1], pts[1:2], grid).astype(BF16)).astype(BF16)
    rows_ref[...] = dot(sy, tent(pts[which : which + 1], pts[which + 1 : which + 2], grid).astype(BF16)).astype(BF16)


def crop_backward_other(points, delta, weight, cells, width):
    count = points.shape[1]
    rois = count // POOL
    channels = weight.shape[0] // BINS

    def body(pts, delta_ref, weight_hbm, crop_ref, out_ref, w_a, w_b, row_ref, col_ref, acc, weight_ref, sems):
        copies = fetch(weight_hbm, weight_ref, sems)
        tables_t(pts, 4, cells, width, row_ref, col_ref)
        for copy in copies:
            copy.wait()
        for i in range(POOL):
            w2 = (w_a, w_b)[i % 2]
            for j in range(POOL):
                k = i * POOL + j
                at = slice(j * rois, (j + 1) * rois)
                w2[:, at] = row_ref[:, i * rois : (i + 1) * rois] * col_ref[:, at]
                crop_ref[k * rois : (k + 1) * rois, :] = dot(
                    delta_ref[...], weight_ref[k * channels : (k + 1) * channels, :], ((1,), (1,))
                ).astype(BF16)
            part = dot(w2[...], crop_ref[i * count : (i + 1) * count, :])
            if i == 0:
                acc[...] = part
            elif i < POOL - 1:
                acc[...] += part
            else:
                out_ref[...] = (acc[...] + part).astype(BF16)

    return kernel(
        body,
        [shaped(BF16, BINS * rois, channels), shaped(BF16, cells, channels)],
        [pltpu.VMEM((cells, count), BF16)] * 4
        + [pltpu.VMEM((cells, channels), F32), pltpu.VMEM(weight.shape, BF16)]
        + [pltpu.SemaphoreType.DMA((POOL,))],
        2 * BINS * rois * cells * channels,
        limit=28,
        anywhere=(2,),
    )(points, delta, weight)


def crop_backward_own(points, crops, cells, width):
    count = points.shape[1]
    rois = count // POOL
    channels = crops.shape[1]

    def body(pts, crop_hbm, acc, w_a, w_b, row_ref, col_ref, crop_ref, sems):
        copies = fetch(crop_hbm, crop_ref, sems)
        tables_t(pts, 2, cells, width, row_ref, col_ref)
        for copy in copies:
            copy.wait()
        for i in range(POOL):
            w2 = (w_a, w_b)[i % 2]
            for j in range(POOL):
                at = slice(j * rois, (j + 1) * rois)
                w2[:, at] = row_ref[:, i * rois : (i + 1) * rois] * col_ref[:, at]
            part = dot(w2[...], crop_ref[i * count : (i + 1) * count, :])
            if i == 0:
                acc[...] = part
            else:
                acc[...] += part

    return kernel(
        body,
        shaped(F32, cells, channels),
        [pltpu.VMEM((cells, count), BF16)] * 4
        + [pltpu.VMEM(crops.shape, BF16), pltpu.SemaphoreType.DMA((POOL,))],
        2 * BINS * rois * cells * channels,
        limit=28,
        anywhere=(1,),
    )(points, crops)


def add_received(own, received):
    def body(own_ref, recv_ref, out_ref):
        out_ref[...] = own_ref[...] + recv_ref[...].astype(F32)

    return kernel(body, shaped(F32, *own.shape), flops=10**8)(own, received)


def weight_grad(packed, deltas, order, me):
    half, width = deltas[0].shape[1:]
    hidden = width // 2
    images, part, lanes = packed.shape
    if lanes == half:
        place = jnp.array([order[m] for m in range(images)])
        in_order = jnp.concatenate(deltas, axis=0)[place[jnp.arange(images) ^ me]]
        total = jnp.einsum("mpr,mrh->ph", packed, in_order, preferred_element_type=F32)
        return total[:, :hidden], total[:, hidden:].astype(BF16)

    def body(me_ref, packed_ref, *refs):
        sources, refs = refs[: len(deltas)], refs[len(deltas) :]
        own_ref, other_ref, *delta_refs, sems = refs
        copies = [
            pltpu.make_async_copy(source, target, sems.at[k])
            for k, (source, target) in enumerate(zip(sources, delta_refs))
        ]
        for copy in copies:
            copy.start()
        for copy in copies:
            copy.wait()
        blocks = [(ref, k) for ref in delta_refs for k in range(ref.shape[0])]
        left = lax.broadcasted_iota(jnp.int32, (part, lanes), 1) < half
        tops = jnp.zeros((part, width), F32)
        bottoms = jnp.zeros((part, width), F32)
        for m in range(0, images, 2):
            a = packed_ref[me_ref[0] ^ m].astype(F32)
            b = packed_ref[me_ref[0] ^ (m + 1)].astype(F32)
            pair = [blocks[order[k]] for k in (m, m + 1)]
            pair = jnp.concatenate([ref[k] for ref, k in pair], axis=0)
            top = jnp.where(left, a, pltpu.roll(b, half, 1)).astype(BF16)
            bottom = jnp.where(left, pltpu.roll(a, half, 1), b).astype(BF16)
            tops += dot(top, pair)
            bottoms += dot(bottom, pair)
        own_ref[:part] = tops[:, :hidden]
        own_ref[part:] = bottoms[:, :hidden]
        other_ref[:part] = tops[:, hidden:].astype(BF16)
        other_ref[part:] = bottoms[:, hidden:].astype(BF16)

    return kernel(
        body,
        [shaped(F32, 2 * part, hidden), shaped(BF16, 2 * part, hidden)],
        [pltpu.VMEM(v.shape, BF16) for v in deltas] + [pltpu.SemaphoreType.DMA((len(deltas),))],
        flops=4 * part * images * half * width,
        limit=16,
        smem_first=True,
        anywhere=range(2, 2 + len(deltas)),
    )(me.reshape(1), packed, *deltas)


def swap_space(values):
    size = lax.axis_size("space")
    return lax.ppermute(values, "space", [(k, size - 1 - k) for k in range(size)])


def swap_images(values, distance):
    return lax.ppermute(values, "dp", [(k, k ^ distance) for k in range(lax.axis_size("dp"))])


def step(feature_map, proposals, hidden_weight, output_weight, upstream):
    images = lax.axis_size("dp")
    assert lax.axis_size("space") == 2 and images & (images - 1) == 0
    bits = images.bit_length() - 1
    own_map = feature_map[0]
    own_height, map_width, channels = own_map.shape
    rois = proposals.shape[1]
    side = lax.axis_index("space")
    me = lax.axis_index("dp").astype(jnp.int32)
    half_cells = own_height * map_width
    padded = -(-half_cells // 128) * 128
    map_own = jnp.pad(own_map.reshape(half_cells, channels), ((0, padded - half_cells), (0, 0)))
    map_other = swap_space(map_own)
    out_other = swap_space(output_weight)

    corners = jnp.roll(proposals[0], side * (rois // 2), axis=0)
    incoming = jnp.roll(upstream[0], side * (rois // 2), axis=0)

    ys = sample_points(corners[:, 0], corners[:, 2])
    xs = sample_points(corners[:, 1], corners[:, 3])
    first_own = (side * own_height).astype(F32)
    first_other = ((1 - side) * own_height).astype(F32)
    points = jnp.stack(
        [p.reshape(-1) for p in xs + [y - f for f in (first_own, first_other) for y in ys]]
    )

    points = jnp.pad(points, ((0, 2), (0, 0)))
    columns = jnp.pad(points.T, ((0, 0), (0, TAPS - points.shape[0])))
    col, row_other, partial = crop_own(columns, map_own, map_width, half_cells)
    pre_hidden, pre_sent, packed = crop_all(
        col, row_other, map_other, partial, hidden_weight, images
    )
    received = lax.all_to_all(packed, "dp", 0, 0, tiled=True)
    pre_other = swap_space(pre_sent)
    delta, mine, second = head(pre_hidden, pre_other, output_weight, out_other, incoming)

    near = [1 << b for b in range(min(2, bits))]
    far = [m for m in range(0, images, 1 << len(near))]
    place = [0]
    gathered = mine[None]
    pieces = [gathered]
    for m in far[1:]:
        pieces.append(swap_images(gathered, m))
    pieces = [jnp.concatenate(pieces, axis=0)]
    place = list(far)
    for distance in near[::-1]:
        pieces = pieces + [swap_images(piece, distance) for piece in pieces]
        place = place + [p ^ distance for p in place]
    order = {m: k for k, m in enumerate(place)}

    crop_grads, grad_other = crop_backward_other(
        points, delta, hidden_weight, half_cells, map_width
    )
    grad_received = swap_space(grad_other)
    grad_own = crop_backward_own(points, crop_grads, half_cells, map_width)
    map_grad = add_received(grad_own, grad_received)
    map_grad = map_grad.reshape(own_height, map_width, channels)

    for distance in near:
        rows = second.shape[0] // 2
        high = (me // distance) % 2
        kept = lax.dynamic_slice_in_dim(second, high * rows, rows, 0)
        sent = lax.dynamic_slice_in_dim(second, (1 - high) * rows, rows, 0)
        theirs = swap_images(sent.astype(BF16), distance)
        second = kept + theirs.astype(F32)
    rounded = second.astype(BF16)
    parts = [rounded] + [swap_images(rounded, m) for m in far[1:]]
    parts = [p.astype(F32) for p in parts]
    while len(parts) > 1:
        parts = [parts[k] + parts[k + 1] for k in range(0, len(parts), 2)]
    second = parts[0]
    second = second.astype(BF16)
    for distance in near[::-1]:
        high = (me // distance) % 2
        theirs = swap_images(second, distance)
        low_part = jnp.where(high == 0, second, theirs)
        high_part = jnp.where(high == 0, theirs, second)
        second = jnp.concatenate([low_part, high_part], axis=0)
    second = second.astype(F32)

    first_own, first_other = weight_grad(received, pieces, order, me)
    first_received = swap_space(first_other)
    return (first_own + first_received.astype(F32), second, map_grad[None])


def solution(mesh):
    placed = (
        P("dp", "space", None, None),
        P("dp", None, None),
        P(None, "space"),
        P("space", None),
        P("dp", None, None),
    )
    return jax.shard_map(
        step,
        mesh=mesh,
        in_specs=placed,
        out_specs=(P("dp", "space"), P("space", None), P("dp", "space", None, None)),
        check_vma=False,
    )
```
